32 devices in a mesh: row: 8 (over z, y), col: 4 (over x, core).
Axes of the slice: x: 2, y: 2, z: 4, core: 2. Of those that a mesh axis runs over, the one named last changes fastest.
Arguments:
- spectra: bfloat16 [1024, 16, 128], P(('row', 'col')), may hold values from -4 to 4
- window_flags: int32 [1024, 64], P(('row', 'col')), may hold values 0 or 1
- pair_mask: int32 [1024, 1024], P('row', 'col'), may hold values 0 or 1
- misfit_weight: bfloat16 [16, 1024, 1024], P(None, 'row', 'col'), may hold values from 0.0099487305 to 0.099609375
- observed: bfloat16 [2, 16, 1024, 1024], P(None, None, 'row', 'col'), may hold values from -6 to 6
Outputs:
- grad_first: bfloat16 [1024, 16, 128], P(('row', 'col'))
- grad_second: bfloat16 [4, 256, 16, 128], P('col', 'row')
The draws below stay inside these ranges and needn't reach their ends.
All inputs are finite; a program needn't handle non-finite values. No bound on the sum of `window_flags` or of `pair_mask` on one device may be relied on, other than what follows from the above.
Results may differ from the reference program's by a relative error of at most 0.019.
Values may be sent and summed in bfloat16 or wider, within the bound.
A program may use at most 64 MiB of HBM per device.

```python
import math
import jax
import jax.numpy as jnp
from jax import lax

ROW_BLOCK = 128
FREQS = 16
WINDOWS = 64
STATIONS = 1024
N_ROW = 8
N_COL = 4


def with_ends(values, stream_key, smallest, largest):
    longest = values.shape.index(max(values.shape))
    spots = []
    for shift in (0, 1):
        where = [jax.random.randint(jax.random.fold_in(stream_key, axis), (), 0, length) for axis, length in enumerate(values.shape)]
        where[longest] = (where[longest] + shift) % values.shape[longest]
        spots.append(tuple(where))
    return values.at[spots[0]].set(smallest).at[spots[1]].set(largest)


def levels(stream_key, shape, split, low, high):
    def one(axis_at, parts):
        heights = jax.random.uniform(jax.random.fold_in(jax.random.fold_in(stream_key, 6), axis_at), (parts,), jnp.float32, low / len(split), high / len(split))
        return jnp.repeat(jnp.exp(heights), shape[axis_at] // parts).reshape((-1,) + (1,) * (len(shape) - axis_at - 1))

    gain = one(*split[0])
    for cut in split[1:]:
        gain = gain * one(*cut)
    return gain


def noise(own_key, dims, deviation, bound, pieces=(), held_as=jnp.bfloat16):
    array = jax.random.normal(own_key, dims, jnp.float32) * deviation
    if len(pieces) > 0:
        array = levels(own_key, dims, pieces, -0.22, 0.18) * array
    return jnp.clip(array, min=-bound, max=bound).astype(held_as)


def setup_inputs(seed: int = 0) -> dict:
    seeds = jax.random.split(jax.random.key(seed), 6)
    spectra = noise(seeds[0], (STATIONS, FREQS, 2 * WINDOWS), 0.3, 4.0, ((0, 32),))
    window_flags = with_ends((jax.random.randint(seeds[1], (STATIONS, WINDOWS), 0, 4) < 3).astype(jnp.int32), jax.random.fold_in(seeds[1], 1), 0, 1)
    pair_mask = with_ends((jax.random.randint(seeds[2], (STATIONS, STATIONS), 0, 5) < 3).astype(jnp.int32), jax.random.fold_in(seeds[2], 1), 0, 1)
    misfit_weight = jnp.clip(jnp.exp(math.log(0.099609375) - 2.3038113 * jax.random.uniform(seeds[3], (FREQS, STATIONS, STATIONS), jnp.float32) ** levels(seeds[3], (FREQS, STATIONS, STATIONS), ((1, 8), (2, 4)), -0.2, 0.2)), 0.0099487305, 0.099609375).astype(jnp.bfloat16)
    observed = noise(seeds[4], (2, FREQS, STATIONS, STATIONS), 1.0, 6.0, ((2, 8), (3, 4)))
    return dict(spectra=spectra, window_flags=window_flags, pair_mask=pair_mask, misfit_weight=misfit_weight, observed=observed)


def reference(spectra, window_flags, pair_mask, misfit_weight, observed):
    half_width = spectra.shape[2] // 2
    flag_value = window_flags.astype(jnp.float32)
    flag_both = jnp.concatenate([flag_value, flag_value], axis=1)
    flagged = (spectra.astype(jnp.float32) * flag_both[:, None, :]).astype(jnp.bfloat16)
    flagged_wide = flagged.astype(jnp.float32)
    swapped = jnp.concatenate([-flagged_wide[..., half_width:], flagged_wide[..., :half_width]], axis=-1)
    col_stack = jnp.stack([flagged_wide, swapped])
    row_stack = jnp.stack([flagged_wide, -swapped])
    col_block = STATIONS // N_COL
    mask_wide = pair_mask.astype(jnp.float32)
    weight_wide = misfit_weight.astype(jnp.float32)
    observed_wide = observed.astype(jnp.float32)
    split_col = col_stack.reshape(2, N_COL, col_block, FREQS, 2 * WINDOWS)

    def one_block(accum_second, block_index):
        first_row = (block_index * ROW_BLOCK).astype(jnp.int32)
        row_part = lax.dynamic_slice_in_dim(flagged_wide, first_row, ROW_BLOCK, 0)
        row_pair = lax.dynamic_slice_in_dim(row_stack, first_row, ROW_BLOCK, 1)
        mask_part = lax.dynamic_slice_in_dim(mask_wide, first_row, ROW_BLOCK, 0)
        weight_part = lax.dynamic_slice_in_dim(weight_wide, first_row, ROW_BLOCK, 1)
        observed_part = lax.dynamic_slice_in_dim(observed_wide, first_row, ROW_BLOCK, 2)
        cross_spec = jnp.einsum('ifk,cjfk->cfij', row_part, col_stack, precision=lax.Precision.HIGHEST)
        residual = (mask_part[None, None] * weight_part[None] * (cross_spec - observed_part)).astype(jnp.bfloat16)
        residual = lax.optimization_barrier(residual).astype(jnp.float32)
        split_res = residual.reshape(2, FREQS, ROW_BLOCK, N_COL, col_block)
        first_terms = jnp.einsum('cfinj,cnjfk->nifk', split_res, split_col, precision=lax.Precision.HIGHEST)
        first_terms = lax.optimization_barrier(first_terms.astype(jnp.bfloat16)).astype(jnp.float32)
        first_grad = jnp.sum(first_terms, axis=0).astype(jnp.bfloat16)
        second_terms = jnp.einsum('cfij,cifk->jfk', residual, row_pair, precision=lax.Precision.HIGHEST)
        second_terms = lax.optimization_barrier(second_terms.astype(jnp.bfloat16)).astype(jnp.float32)
        return accum_second + second_terms, first_grad

    initial = jnp.zeros((STATIONS, FREQS, 2 * WINDOWS), jnp.float32)
    accum_second, firsts = lax.scan(one_block, initial, jnp.arange(N_ROW, dtype=jnp.int32))
    grad_first = firsts.reshape(STATIONS, FREQS, 2 * WINDOWS)
    grad_second = accum_second.astype(jnp.bfloat16).reshape(N_COL, col_block, FREQS, 2 * WINDOWS)
    return grad_first, grad_second
```

```python
import functools

import jax
import jax.numpy as jnp
from jax import lax
from jax.experimental import pallas as pl
from jax.experimental.pallas import tpu as pltpu
from jax.sharding import PartitionSpec as P

MESH = pl.DeviceIdType.MESH
GROUP = 2


def plain(fn):
    return fn()


def kernel(
    n_row, n_col, chunks, group,
    own, mask, w_hbm, obs_hbm, out_first, out_second,
    v1, v2, w_v, obs_v, gf, gf_sum, rc, rx, gs, gs_sum, ry, rz,
    in_sem, own_sem, xs, xr, ds, dr, zs, zr, ys, yr,
    cs, cr, ps, pr, hs, hr, qs, qr,
):
    ratio = n_row // n_col
    n_z = n_row // ratio
    n_x = n_col // 2
    row, col = lax.axis_index("row"), lax.axis_index("col")
    z, y = row // ratio, row % ratio
    x, core = col // 2, col % 2
    shard = own.shape[1]
    first_rows = n_col * shard
    second_rows = ratio * first_rows
    half = own.shape[2] // 2

    def col_at(step):
        return ((x + step) % n_x) * 2 + core

    partner = x * 2 + (1 - core)

    def row_y(step):
        return z * ratio + (y + step) % ratio

    def row_z(step):
        return ((z + step) % n_z) * ratio + y

    def span(k):
        return pl.ds(k * group, group)

    def remote(src, dst, ssem, rsem, to_row, to_col):
        return pltpu.make_async_remote_copy(
            src_ref=src, dst_ref=dst, send_sem=ssem, recv_sem=rsem,
            device_id=(to_row, to_col), device_id_type=MESH,
        )

    def send_x(k, d):
        return remote(own.at[span(k)], v1.at[span(k), col], xs.at[d - 1, k], xr.at[d - 1, k], row, col_at(d))

    def send_d(k, d):
        if d == 0:
            return remote(own.at[span(k)], v1.at[span(k), col], ds.at[0, k], dr.at[0, k], row, partner)
        piece = v1.at[span(k), col_at(n_x - d)]
        return remote(piece, piece, ds.at[d, k], dr.at[d, k], row, partner)

    def send_z(k, up, src):
        to = (z + 1 if up else z - 1) * ratio + y
        return remote(src, v2.at[span(k), y], zs.at[0 if up else 1, k], zr.at[k], to, col)

    def send_y(k, d, src):
        return remote(src, v2.at[span(k), y], ys.at[d - 1, k], yr.at[d - 1, k], row_y(d), col)

    def send_c(k):
        return remote(gf.at[span(k), :, 1 - core], rc.at[span(k)], cs.at[k], cr.at[k], row, partner)

    def send_p(k, d):
        return remote(gf_sum.at[span(k), (x + d) % n_x], rx.at[d - 1, span(k)], ps.at[d - 1, k], pr.at[d - 1, k], row, col_at(d))

    def send_h(k, d):
        return remote(gs.at[span(k), :, (y + d) % ratio], ry.at[d - 1, span(k)], hs.at[d - 1, k], hr.at[d - 1, k], row_y(d), col)

    def send_q(k, d):
        return remote(gs_sum.at[span(k), (z + d) % n_z], rz.at[d - 1, span(k)], qs.at[d - 1, k], qr.at[d - 1, k], row_z(d), col)

    home = z == col
    up_ok = jnp.logical_and(z >= col, z + 1 < n_z)
    down_ok = jnp.logical_and(z <= col, z >= 1)

    load_w = pltpu.make_async_copy(w_hbm, w_v, in_sem.at[0])
    load_obs = pltpu.make_async_copy(obs_hbm, obs_v, in_sem.at[1])
    load_own = pltpu.make_async_copy(own, v1.at[:, col], own_sem)
    load_w.start()
    load_obs.start()
    load_own.start()

    barrier = pltpu.get_barrier_semaphore()
    peers = [(row, partner)]
    peers += [(row, col_at(d)) for d in range(1, n_x)]
    peers += [(row_y(d), col) for d in range(1, ratio)]
    peers += [(row_z(d), col) for d in range(1, n_z)]
    for peer in peers:
        pl.semaphore_signal(barrier, inc=1, device_id=peer, device_id_type=MESH)
    pl.semaphore_wait(barrier, len(peers))

    @pl.loop(0, chunks)
    def _(k):
        for d in range(1, n_x):
            send_x(k, d).start()
        send_d(k, 0).start()

    load_own.wait()

    def forward(k, src):
        @pl.when(up_ok)
        def _():
            send_z(k, True, src).start()

        @pl.when(down_ok)
        def _():
            send_z(k, False, src).start()

        for d in range(1, ratio):
            send_y(k, d, src).start()

    @pl.loop(0, chunks + 1)
    def _(it):
        @pl.when(it < chunks)
        def _():
            for d in range(1, n_x):
                send_x(it, d).wait_recv()
                send_d(it, d).start()

        @pl.when(it >= 1)
        def _():
            k = it - 1
            for d in range(n_x):
                send_d(k, d).wait_recv()

            @pl.when(home)
            def _():
                forward(k, v1.at[span(k)])
                pltpu.make_async_copy(v1.at[span(k)], v2.at[span(k), y], zr.at[k]).start()

    load_w.wait()
    load_obs.wait()

    lane = lax.broadcasted_iota(jnp.int32, (1, 2 * half), 1)
    low_plus = jnp.where(lane < half, 1.0, -1.0).astype(jnp.float32)

    def compute(f):
        a = v1[f].astype(jnp.float32).reshape(first_rows, 2 * half)
        b = v2[f].astype(jnp.float32).reshape(second_rows, 2 * half).astype(jnp.bfloat16)
        turned = pltpu.roll(a, half, 1) * low_plus
        w = jnp.concatenate([a, turned], axis=0).astype(jnp.bfloat16)
        cross = lax.dot_general(w, b, (((1,), (1,)), ((), ())), preferred_element_type=jnp.float32)
        scale = mask[...].astype(jnp.float32) * w_v[f].astype(jnp.float32)
        res = jnp.concatenate(
            [
                (scale * (cross[:first_rows] - obs_v[0, f].astype(jnp.float32))).astype(jnp.bfloat16),
                (scale * (cross[first_rows:] - obs_v[1, f].astype(jnp.float32))).astype(jnp.bfloat16),
            ],
            axis=0,
        )
        t = jnp.dot(res, b, preferred_element_type=jnp.float32)
        g1 = t[:first_rows] - pltpu.roll(t[first_rows:], half, 1) * low_plus
        gf[f] = g1.reshape(n_x, 2, shard, 2 * half).astype(jnp.bfloat16)
        g2 = lax.dot_general(res, w, (((0,), (0,)), ((), ())), preferred_element_type=jnp.float32)
        gs[f] = g2.reshape(n_z, ratio, shard, 2 * half).astype(jnp.bfloat16)

    lag_y, lag_h, lag_c = 1, 3, 4

    @pl.loop(0, chunks + lag_c)
    def _(it):
        @pl.when(it < chunks)
        def _():
            pltpu.make_async_copy(v1.at[span(it)], v2.at[span(it), y], zr.at[it]).wait()

            @pl.when(jnp.logical_not(home))
            def _():
                forward(it, v2.at[span(it), y])

        @pl.when(jnp.logical_and(it >= lag_y, it < chunks + lag_y))
        def _():
            k = it - lag_y
            for d in range(1, ratio):
                send_y(k, d, v2.at[span(k), y]).wait_recv()
            for i in range(group):
                compute(k * group + i)
            send_c(k).start()
            for d in range(1, ratio):
                send_h(k, d).start()

        @pl.when(jnp.logical_and(it >= lag_h, it < chunks + lag_h))
        def _():
            k = it - lag_h
            for d in range(1, ratio):
                send_h(k, d).wait_recv()
            total = gs[span(k), :, y].astype(jnp.float32)
            for d in range(1, ratio):
                total = total + ry[d - 1, span(k)].astype(jnp.float32)
            gs_sum[span(k)] = total.astype(jnp.bfloat16)
            for d in range(1, n_z):
                send_q(k, d).start()

        @pl.when(it >= lag_c)
        def _():
            k = it - lag_c
            send_c(k).wait_recv()
            total = gf[span(k), :, core].astype(jnp.float32) + rc[span(k)].astype(jnp.float32)
            gf_sum[span(k)] = total.astype(jnp.bfloat16)
            for d in range(1, n_x):
                send_p(k, d).start()

    @pl.loop(0, chunks)
    def _(k):
        for d in range(1, n_x):
            send_p(k, d).wait_recv()
        total = gf_sum[span(k), x].astype(jnp.float32)
        for d in range(1, n_x):
            total = total + rx[d - 1, span(k)].astype(jnp.float32)
        out_first[span(k)] = total.astype(jnp.bfloat16)
        for d in range(1, n_z):
            send_q(k, d).wait_recv()
        total = gs_sum[span(k), z].astype(jnp.float32)
        for d in range(1, n_z):
            total = total + rz[d - 1, span(k)].astype(jnp.float32)
        out_second[span(k)] = total.astype(jnp.bfloat16)

    @pl.loop(0, chunks)
    def _(k):
        for d in range(1, n_x):
            send_x(k, d).wait_send()
            send_p(k, d).wait_send()
        for d in range(n_x):
            send_d(k, d).wait_send()
        src = v1.at[span(k)]

        @pl.when(up_ok)
        def _():
            send_z(k, True, src).wait_send()

        @pl.when(down_ok)
        def _():
            send_z(k, False, src).wait_send()

        for d in range(1, ratio):
            send_y(k, d, src).wait_send()
            send_h(k, d).wait_send()
        send_c(k).wait_send()
        for d in range(1, n_z):
            send_q(k, d).wait_send()


def per_device(n_row, n_col, spectra, window_flags, pair_mask, misfit_weight, observed):
    shard, freqs, width = spectra.shape
    ratio = n_row // n_col
    n_z, n_x = n_row // ratio, n_col // 2
    group = GROUP if freqs % GROUP == 0 else 1
    chunks = freqs // group
    flag_value = window_flags.astype(jnp.bfloat16)
    flag_both = jnp.concatenate([flag_value, flag_value], axis=1)
    own = jnp.transpose(spectra * flag_both[:, None, :], (1, 0, 2))
    bf = jnp.bfloat16
    vm = lambda *shape: pltpu.VMEM(shape, bf)
    dma = lambda *shape: pltpu.SemaphoreType.DMA(shape)
    first, second = pl.pallas_call(
        functools.partial(kernel, n_row, n_col, chunks, group),
        out_shape=[jax.ShapeDtypeStruct((freqs, shard, width), bf)] * 2,
        in_specs=[
            pl.BlockSpec(memory_space=pltpu.VMEM),
            pl.BlockSpec(memory_space=pltpu.VMEM),
            pl.BlockSpec(memory_space=pl.ANY),
            pl.BlockSpec(memory_space=pl.ANY),
        ],
        out_specs=[pl.BlockSpec(memory_space=pltpu.VMEM)] * 2,
        scratch_shapes=[
            vm(freqs, n_col, shard, width),
            vm(freqs, ratio, n_col, shard, width),
            pltpu.VMEM(misfit_weight.shape, bf),
            pltpu.VMEM(observed.shape, bf),
            vm(freqs, n_x, 2, shard, width),
            vm(freqs, n_x, shard, width),
            vm(freqs, n_x, shard, width),
            vm(n_x - 1, freqs, shard, width),
            vm(freqs, n_z, ratio, shard, width),
            vm(freqs, n_z, shard, width),
            vm(ratio - 1, freqs, n_z, shard, width),
            vm(n_z - 1, freqs, shard, width),
            dma(2), pltpu.SemaphoreType.DMA,
            dma(n_x - 1, chunks), dma(n_x - 1, chunks),
            dma(n_x, chunks), dma(n_x, chunks),
            dma(2, chunks), dma(chunks),
            dma(ratio - 1, chunks), dma(ratio - 1, chunks),
            dma(chunks), dma(chunks),
            dma(n_x - 1, chunks), dma(n_x - 1, chunks),
            dma(ratio - 1, chunks), dma(ratio - 1, chunks),
            dma(n_z - 1, chunks), dma(n_z - 1, chunks),
        ],
        compiler_params=pltpu.CompilerParams(collective_id=0, has_side_effects=True),
        name="adjoint",
    )(own, pair_mask, misfit_weight, observed)
    return jnp.transpose(first, (1, 0, 2)), jnp.transpose(second, (1, 0, 2))[None]


def solution(mesh):
    placed = (
        P(("row", "col"), None, None),
        P(("row", "col"), None),
        P("row", "col"),
        P(None, "row", "col"),
        P(None, None, "row", "col"),
    )
    return jax.shard_map(
        functools.partial(per_device, mesh.shape["row"], mesh.shape["col"]),
        mesh=mesh,
        in_specs=placed,
        out_specs=(P(("row", "col"), None, None), P("col", "row", None, None)),
        check_vma=False,
    )
```

```python
import functools

import jax
import jax.numpy as jnp
from jax import lax
from jax.experimental import pallas as pl
from jax.experimental.pallas import tpu as pltpu
from jax.sharding import PartitionSpec as P

MESH = pl.DeviceIdType.MESH
GROUP = 2


def kernel(
    n_row, n_col, chunks, group,
    own, mask, w_hbm, obs_hbm, out_first, out_second,
    v1, v2, w_v, obs_v, gf, gf_sum, rc, rx, gs, gs_sum, ry, rz,
    in_sem, own_sem, fs, fr, zs, zr, lz, ys, yr,
    cs, cr, ps, pr, hs, hr, qs, qr,
):
    ratio = n_row // n_col
    n_z = n_row // ratio
    n_x = n_col // 2
    row, col = lax.axis_index("row"), lax.axis_index("col")
    z, y = row // ratio, row % ratio
    x, core = col // 2, col % 2
    shard = own.shape[1]
    first_rows = n_col * shard
    second_rows = ratio * first_rows
    half = own.shape[2] // 2

    def col_at(step):
        return ((x + step) % n_x) * 2 + core

    partner = x * 2 + (1 - core)

    def row_y(step):
        return z * ratio + (y + step) % ratio

    def row_z(step):
        return ((z + step) % n_z) * ratio + y

    def span(k):
        return pl.ds(k * group, group)

    def remote(src, dst, ssem, rsem, to_row, to_col):
        return pltpu.make_async_remote_copy(
            src_ref=src, dst_ref=dst, send_sem=ssem, recv_sem=rsem,
            device_id=(to_row, to_col), device_id_type=MESH,
        )

    def send_f(k, d):
        return remote(own.at[span(k)], v1.at[span(k), col], fs.at[d - 1, k], fr.at[d - 1, k], row, (col + d) % n_col)

    def send_z(k, d):
        return remote(own.at[span(k)], v2.at[span(k), y, col], zs.at[d - 1, k], zr.at[col, k], row_z(d), z)

    def send_y(k, d, src):
        return remote(src, v2.at[span(k), y], ys.at[d - 1, k], yr.at[d - 1, k], row_y(d), col)

    def send_c(k):
        return remote(gf.at[span(k), :, 1 - core], rc.at[span(k)], cs.at[k], cr.at[k], row, partner)

    def send_p(k, d):
        return remote(gf_sum.at[span(k), (x + d) % n_x], rx.at[d - 1, span(k)], ps.at[d - 1, k], pr.at[d - 1, k], row, col_at(d))

    def send_h(k, d):
        return remote(gs.at[span(k), :, (y + d) % ratio], ry.at[d - 1, span(k)], hs.at[d - 1, k], hr.at[d - 1, k], row_y(d), col)

    def send_q(k, d):
        return remote(gs_sum.at[span(k), (z + d) % n_z], rz.at[d - 1, span(k)], qs.at[d - 1, k], qr.at[d - 1, k], row_z(d), col)

    home = z == col

    load_w = pltpu.make_async_copy(w_hbm, w_v, in_sem.at[0])
    load_obs = pltpu.make_async_copy(obs_hbm, obs_v, in_sem.at[1])
    load_own = pltpu.make_async_copy(own, v1.at[:, col], own_sem)
    load_w.start()
    load_obs.start()
    load_own.start()

    barrier = pltpu.get_barrier_semaphore()

    def tell(to_row, to_col):
        pl.semaphore_signal(barrier, inc=1, device_id=(to_row, to_col), device_id_type=MESH)

    @pl.when(jnp.logical_not(home))
    def _():
        for j in range(n_col):
            tell(col * ratio + y, j)

    for d in range(1, n_z):
        tell(row_z(d), col)
    for d in range(1, ratio):
        tell(row_y(d), col)
    for d in range(1, n_col):
        tell(row, (col + d) % n_col)
    pl.semaphore_wait(barrier, n_col - 1 + 2 * (n_z - 1) + ratio - 1)

    @pl.loop(0, chunks)
    def _(k):
        for d in range(1, n_z):
            send_z(k, d).start()
        for d in range(1, n_col):
            send_f(k, d).start()

    load_own.wait()

    def wait_first(k):
        for d in range(1, n_col):
            send_f(k, d).wait_recv()

    def local_copy(k):
        return pltpu.make_async_copy(v1.at[span(k)], v2.at[span(k), y], lz.at[k])

    load_w.wait()
    load_obs.wait()

    lane = lax.broadcasted_iota(jnp.int32, (1, 2 * half), 1)
    low_plus = jnp.where(lane < half, 1.0, -1.0).astype(jnp.float32)

    def compute(f):
        a = v1[f].astype(jnp.float32).reshape(first_rows, 2 * half)
        b = v2[f].astype(jnp.float32).reshape(second_rows, 2 * half).astype(jnp.bfloat16)
        turned = pltpu.roll(a, half, 1) * low_plus
        w = jnp.concatenate([a, turned], axis=0).astype(jnp.bfloat16)
        cross = lax.dot_general(w, b, (((1,), (1,)), ((), ())), preferred_element_type=jnp.float32)
        scale = mask[...].astype(jnp.float32) * w_v[f].astype(jnp.float32)
        res = jnp.concatenate(
            [
                (scale * (cross[:first_rows] - obs_v[0, f].astype(jnp.float32))).astype(jnp.bfloat16),
                (scale * (cross[first_rows:] - obs_v[1, f].astype(jnp.float32))).astype(jnp.bfloat16),
            ],
            axis=0,
        )
        t = jnp.dot(res, b, preferred_element_type=jnp.float32)
        g1 = t[:first_rows] - pltpu.roll(t[first_rows:], half, 1) * low_plus
        gf[f] = g1.reshape(n_x, 2, shard, 2 * half).astype(jnp.bfloat16)
        g2 = lax.dot_general(res, w, (((0,), (0,)), ((), ())), preferred_element_type=jnp.float32)
        gs[f] = g2.reshape(n_z, ratio, shard, 2 * half).astype(jnp.bfloat16)

    lag_y, lag_h, lag_c = 2, 4, 5

    @pl.loop(0, chunks + lag_c)
    def _(it):
        @pl.when(it < chunks)
        def _():
            @pl.when(home)
            def _():
                wait_first(it)
                for d in range(1, ratio):
                    send_y(it, d, v1.at[span(it)]).start()
                local_copy(it).start()

            @pl.when(jnp.logical_not(home))
            def _():
                for j in range(n_col):
                    remote(own.at[span(it)], v2.at[span(it), y, j], zs.at[0, it], zr.at[j, it], row, col).wait_recv()
                for d in range(1, ratio):
                    send_y(it, d, v2.at[span(it), y]).start()

        @pl.when(jnp.logical_and(it >= lag_y, it < chunks + lag_y))
        def _():
            k = it - lag_y
            for d in range(1, ratio):
                send_y(k, d, v2.at[span(k), y]).wait_recv()

            @pl.when(home)
            def _():
                local_copy(k).wait()

            @pl.when(jnp.logical_not(home))
            def _():
                wait_first(k)

            for i in range(group):
                compute(k * group + i)
            send_c(k).start()
            for d in range(1, ratio):
                send_h(k, d).start()

        @pl.when(jnp.logical_and(it >= lag_h, it < chunks + lag_h))
        def _():
            k = it - lag_h
            for d in range(1, ratio):
                send_h(k, d).wait_recv()
            total = gs[span(k), :, y].astype(jnp.float32)
            for d in range(1, ratio):
                total = total + ry[d - 1, span(k)].astype(jnp.float32)
            gs_sum[span(k)] = total.astype(jnp.bfloat16)
            for d in range(1, n_z):
                send_q(k, d).start()

        @pl.when(it >= lag_c)
        def _():
            k = it - lag_c
            send_c(k).wait_recv()
            total = gf[span(k), :, core].astype(jnp.float32) + rc[span(k)].astype(jnp.float32)
            gf_sum[span(k)] = total.astype(jnp.bfloat16)
            for d in range(1, n_x):
                send_p(k, d).start()

    @pl.loop(0, chunks)
    def _(k):
        for d in range(1, n_x):
            send_p(k, d).wait_recv()
        total = gf_sum[span(k), x].astype(jnp.float32)
        for d in range(1, n_x):
            total = total + rx[d - 1, span(k)].astype(jnp.float32)
        out_first[span(k)] = total.astype(jnp.bfloat16)
        for d in range(1, n_z):
            send_q(k, d).wait_recv()
        total = gs_sum[span(k), z].astype(jnp.float32)
        for d in range(1, n_z):
            total = total + rz[d - 1, span(k)].astype(jnp.float32)
        out_second[span(k)] = total.astype(jnp.bfloat16)

    @pl.loop(0, chunks)
    def _(k):
        for d in range(1, n_x):
            send_p(k, d).wait_send()
        for d in range(1, n_col):
            send_f(k, d).wait_send()
        for d in range(1, ratio):
            send_y(k, d, v1.at[span(k)]).wait_send()
            send_h(k, d).wait_send()
        send_c(k).wait_send()
        for d in range(1, n_z):
            send_z(k, d).wait_send()
            send_q(k, d).wait_send()


def per_device(n_row, n_col, spectra, window_flags, pair_mask, misfit_weight, observed):
    shard, freqs, width = spectra.shape
    ratio = n_row // n_col
    n_z, n_x = n_row // ratio, n_col // 2
    group = GROUP if freqs % GROUP == 0 else 1
    chunks = freqs // group
    flag_value = window_flags.astype(jnp.bfloat16)
    flag_both = jnp.concatenate([flag_value, flag_value], axis=1)
    own = jnp.transpose(spectra * flag_both[:, None, :], (1, 0, 2))
    bf = jnp.bfloat16
    vm = lambda *shape: pltpu.VMEM(shape, bf)
    dma = lambda *shape: pltpu.SemaphoreType.DMA(shape)
    first, second = pl.pallas_call(
        functools.partial(kernel, n_row, n_col, chunks, group),
        out_shape=[jax.ShapeDtypeStruct((freqs, shard, width), bf)] * 2,
        in_specs=[
            pl.BlockSpec(memory_space=pltpu.VMEM),
            pl.BlockSpec(memory_space=pltpu.VMEM),
            pl.BlockSpec(memory_space=pl.ANY),
            pl.BlockSpec(memory_space=pl.ANY),
        ],
        out_specs=[pl.BlockSpec(memory_space=pltpu.VMEM)] * 2,
        scratch_shapes=[
            vm(freqs, n_col, shard, width),
            vm(freqs, ratio, n_col, shard, width),
            pltpu.VMEM(misfit_weight.shape, bf),
            pltpu.VMEM(observed.shape, bf),
            vm(freqs, n_x, 2, shard, width),
            vm(freqs, n_x, shard, width),
            vm(freqs, n_x, shard, width),
            vm(n_x - 1, freqs, shard, width),
            vm(freqs, n_z, ratio, shard, width),
            vm(freqs, n_z, shard, width),
            vm(ratio - 1, freqs, n_z, shard, width),
            vm(n_z - 1, freqs, shard, width),
            dma(2), pltpu.SemaphoreType.DMA,
            dma(n_col - 1, chunks), dma(n_col - 1, chunks),
            dma(n_z - 1, chunks), dma(n_col, chunks), dma(chunks),
            dma(ratio - 1, chunks), dma(ratio - 1, chunks),
            dma(chunks), dma(chunks),
            dma(n_x - 1, chunks), dma(n_x - 1, chunks),
            dma(ratio - 1, chunks), dma(ratio - 1, chunks),
            dma(n_z - 1, chunks), dma(n_z - 1, chunks),
        ],
        compiler_params=pltpu.CompilerParams(collective_id=0, has_side_effects=True),
        name="adjoint",
    )(own, pair_mask, misfit_weight, observed)
    return jnp.transpose(first, (1, 0, 2)), jnp.transpose(second, (1, 0, 2))[None]


def solution(mesh):
    placed = (
        P(("row", "col"), None, None),
        P(("row", "col"), None),
        P("row", "col"),
        P(None, "row", "col"),
        P(None, None, "row", "col"),
    )
    return jax.shard_map(
        functools.partial(per_device, mesh.shape["row"], mesh.shape["col"]),
        mesh=mesh,
        in_specs=placed,
        out_specs=(P(("row", "col"), None, None), P("col", "row", None, None)),
        check_vma=False,
    )
```

```python
import functools

import jax
import jax.numpy as jnp
from jax import lax
from jax.experimental import pallas as pl
from jax.experimental.pallas import tpu as pltpu
from jax.sharding import PartitionSpec as P

MESH = pl.DeviceIdType.MESH
GROUP = 2


def kernel(
    n_row, n_col, chunks, group,
    raw, flags, mask, w_hbm, obs_hbm, out_first, out_second,
    own,
    v1, v2, w_v, obs_v, gf, gf_sum, rc, rx, gs, gs_sum, ry, rz,
    in_sem, own_sem, fs, fr, zs, zr, lz, ys, yr,
    cs, cr, ps, pr, hs, hr, qs, qr,
):
    ratio = n_row // n_col
    n_z = n_row // ratio
    n_x = n_col // 2
    row, col = lax.axis_index("row"), lax.axis_index("col")
    z, y = row // ratio, row % ratio
    x, core = col // 2, col % 2
    shard = own.shape[1]
    first_rows = n_col * shard
    second_rows = ratio * first_rows
    half = own.shape[2] // 2

    def col_at(step):
        return ((x + step) % n_x) * 2 + core

    partner = x * 2 + (1 - core)

    def row_y(step):
        return z * ratio + (y + step) % ratio

    def row_z(step):
        return ((z + step) % n_z) * ratio + y

    def span(k):
        return pl.ds(k * group, group)

    def remote(src, dst, ssem, rsem, to_row, to_col):
        return pltpu.make_async_remote_copy(
            src_ref=src, dst_ref=dst, send_sem=ssem, recv_sem=rsem,
            device_id=(to_row, to_col), device_id_type=MESH,
        )

    def send_f(k, d):
        return remote(own.at[span(k)], v1.at[span(k), col], fs.at[d - 1, k], fr.at[d - 1, k], row, (col + d) % n_col)

    def send_z(k, d):
        return remote(own.at[span(k)], v2.at[span(k), y, col], zs.at[d - 1, k], zr.at[col, k], row_z(d), z)

    def send_y(k, d, src):
        return remote(src, v2.at[span(k), y], ys.at[d - 1, k], yr.at[d - 1, k], row_y(d), col)

    def send_c(k):
        return remote(gf.at[span(k), :, 1 - core], rc.at[span(k)], cs.at[k], cr.at[k], row, partner)

    def send_p(k, d):
        return remote(gf_sum.at[span(k), (x + d) % n_x], rx.at[d - 1, span(k)], ps.at[d - 1, k], pr.at[d - 1, k], row, col_at(d))

    def send_h(k, d):
        return remote(gs.at[span(k), :, (y + d) % ratio], ry.at[d - 1, span(k)], hs.at[d - 1, k], hr.at[d - 1, k], row_y(d), col)

    def send_q(k, d):
        return remote(gs_sum.at[span(k), (z + d) % n_z], rz.at[d - 1, span(k)], qs.at[d - 1, k], qr.at[d - 1, k], row_z(d), col)

    home = z == col

    load_w = pltpu.make_async_copy(w_hbm, w_v, in_sem.at[0])
    load_obs = pltpu.make_async_copy(obs_hbm, obs_v, in_sem.at[1])
    load_own = pltpu.make_async_copy(own, v1.at[:, col], own_sem)
    load_w.start()
    load_obs.start()

    barrier = pltpu.get_barrier_semaphore()

    def tell(to_row, to_col):
        pl.semaphore_signal(barrier, inc=1, device_id=(to_row, to_col), device_id_type=MESH)

    @pl.when(jnp.logical_not(home))
    def _():
        for j in range(n_col):
            tell(col * ratio + y, j)

    for d in range(1, n_z):
        tell(row_z(d), col)
    for d in range(1, ratio):
        tell(row_y(d), col)
    for d in range(1, n_col):
        tell(row, (col + d) % n_col)

    flag_value = flags[...].astype(jnp.float32)
    flag_both = jnp.concatenate([flag_value, flag_value], axis=1)
    flagged = raw[...].astype(jnp.float32) * flag_both[:, None, :]
    own[...] = jnp.transpose(flagged, (1, 0, 2)).astype(jnp.bfloat16)
    load_own.start()
    pl.semaphore_wait(barrier, n_col - 1 + 2 * (n_z - 1) + ratio - 1)

    @pl.loop(0, chunks)
    def _(k):
        for d in range(1, n_z):
            send_z(k, d).start()
        for d in range(1, n_col):
            send_f(k, d).start()

    load_own.wait()

    def wait_first(k):
        for d in range(1, n_col):
            send_f(k, d).wait_recv()

    def local_copy(k):
        return pltpu.make_async_copy(v1.at[span(k)], v2.at[span(k), y], lz.at[k])

    load_w.wait()
    load_obs.wait()

    lane = lax.broadcasted_iota(jnp.int32, (1, 2 * half), 1)
    low_plus = jnp.where(lane < half, 1.0, -1.0).astype(jnp.float32)

    def compute(f):
        a = v1[f].astype(jnp.float32).reshape(first_rows, 2 * half)
        b = v2[f].astype(jnp.float32).reshape(second_rows, 2 * half).astype(jnp.bfloat16)
        turned = pltpu.roll(a, half, 1) * low_plus
        w = jnp.concatenate([a, turned], axis=0).astype(jnp.bfloat16)
        cross = lax.dot_general(w, b, (((1,), (1,)), ((), ())), preferred_element_type=jnp.float32)
        scale = mask[...].astype(jnp.float32) * w_v[f].astype(jnp.float32)
        res = jnp.concatenate(
            [
                (scale * (cross[:first_rows] - obs_v[0, f].astype(jnp.float32))).astype(jnp.bfloat16),
                (scale * (cross[first_rows:] - obs_v[1, f].astype(jnp.float32))).astype(jnp.bfloat16),
            ],
            axis=0,
        )
        t = jnp.dot(res, b, preferred_element_type=jnp.float32)
        g1 = t[:first_rows] - pltpu.roll(t[first_rows:], half, 1) * low_plus
        gf[f] = g1.reshape(n_x, 2, shard, 2 * half).astype(jnp.bfloat16)
        g2 = lax.dot_general(res, w, (((0,), (0,)), ((), ())), preferred_element_type=jnp.float32)
        gs[f] = g2.reshape(n_z, ratio, shard, 2 * half).astype(jnp.bfloat16)

    lag_y, lag_h, lag_c = 2, 4, 5

    @pl.loop(0, chunks + lag_c)
    def _(it):
        @pl.when(it < chunks)
        def _():
            @pl.when(home)
            def _():
                wait_first(it)
                for d in range(1, ratio):
                    send_y(it, d, v1.at[span(it)]).start()
                local_copy(it).start()

            @pl.when(jnp.logical_not(home))
            def _():
                for j in range(n_col):
                    remote(own.at[span(it)], v2.at[span(it), y, j], zs.at[0, it], zr.at[j, it], row, col).wait_recv()
                for d in range(1, ratio):
                    send_y(it, d, v2.at[span(it), y]).start()

        @pl.when(jnp.logical_and(it >= lag_y, it < chunks + lag_y))
        def _():
            k = it - lag_y
            for d in range(1, ratio):
                send_y(k, d, v2.at[span(k), y]).wait_recv()

            @pl.when(home)
            def _():
                local_copy(k).wait()

            @pl.when(jnp.logical_not(home))
            def _():
                wait_first(k)

            for i in range(group):
                compute(k * group + i)
            send_c(k).start()
            for d in range(1, ratio):
                send_h(k, d).start()

        @pl.when(jnp.logical_and(it >= lag_h, it < chunks + lag_h))
        def _():
            k = it - lag_h
            for d in range(1, ratio):
                send_h(k, d).wait_recv()
            total = gs[span(k), :, y].astype(jnp.float32)
            for d in range(1, ratio):
                total = total + ry[d - 1, span(k)].astype(jnp.float32)
            gs_sum[span(k)] = total.astype(jnp.bfloat16)
            for d in range(1, n_z):
                send_q(k, d).start()

        @pl.when(it >= lag_c)
        def _():
            k = it - lag_c
            send_c(k).wait_recv()
            total = gf[span(k), :, core].astype(jnp.float32) + rc[span(k)].astype(jnp.float32)
            gf_sum[span(k)] = total.astype(jnp.bfloat16)
            for d in range(1, n_x):
                send_p(k, d).start()

    @pl.loop(0, chunks)
    def _(k):
        for d in range(1, n_x):
            send_p(k, d).wait_recv()
        total = gf_sum[span(k), x].astype(jnp.float32)
        for d in range(1, n_x):
            total = total + rx[d - 1, span(k)].astype(jnp.float32)
        out_first[span(k)] = total.astype(jnp.bfloat16)
        for d in range(1, n_z):
            send_q(k, d).wait_recv()
        total = gs_sum[span(k), z].astype(jnp.float32)
        for d in range(1, n_z):
            total = total + rz[d - 1, span(k)].astype(jnp.float32)
        out_second[span(k)] = total.astype(jnp.bfloat16)

    @pl.loop(0, chunks)
    def _(k):
        for d in range(1, n_x):
            send_p(k, d).wait_send()
        for d in range(1, n_col):
            send_f(k, d).wait_send()
        for d in range(1, ratio):
            send_y(k, d, v1.at[span(k)]).wait_send()
            send_h(k, d).wait_send()
        send_c(k).wait_send()
        for d in range(1, n_z):
            send_z(k, d).wait_send()
            send_q(k, d).wait_send()


def turn_kernel(first, second, out_first, out_second):
    for src, dst in ((first, out_first), (second, out_second)):
        dst[...] = jnp.transpose(src[...].astype(jnp.float32), (1, 0, 2)).astype(jnp.bfloat16)


def per_device(n_row, n_col, spectra, window_flags, pair_mask, misfit_weight, observed):
    shard, freqs, width = spectra.shape
    ratio = n_row // n_col
    n_z, n_x = n_row // ratio, n_col // 2
    group = GROUP if freqs % GROUP == 0 else 1
    chunks = freqs // group
    bf = jnp.bfloat16
    vm = lambda *shape: pltpu.VMEM(shape, bf)
    dma = lambda *shape: pltpu.SemaphoreType.DMA(shape)
    first, second = pl.pallas_call(
        functools.partial(kernel, n_row, n_col, chunks, group),
        out_shape=[jax.ShapeDtypeStruct((freqs, shard, width), bf)] * 2,
        in_specs=[
            pl.BlockSpec(memory_space=pltpu.VMEM),
            pl.BlockSpec(memory_space=pltpu.VMEM),
            pl.BlockSpec(memory_space=pltpu.VMEM),
            pl.BlockSpec(memory_space=pl.ANY),
            pl.BlockSpec(memory_space=pl.ANY),
        ],
        out_specs=[pl.BlockSpec(memory_space=pltpu.VMEM)] * 2,
        scratch_shapes=[
            vm(freqs, shard, width),
            vm(freqs, n_col, shard, width),
            vm(freqs, ratio, n_col, shard, width),
            pltpu.VMEM(misfit_weight.shape, bf),
            pltpu.VMEM(observed.shape, bf),
            vm(freqs, n_x, 2, shard, width),
            vm(freqs, n_x, shard, width),
            vm(freqs, n_x, shard, width),
            vm(n_x - 1, freqs, shard, width),
            vm(freqs, n_z, ratio, shard, width),
            vm(freqs, n_z, shard, width),
            vm(ratio - 1, freqs, n_z, shard, width),
            vm(n_z - 1, freqs, shard, width),
            dma(2), pltpu.SemaphoreType.DMA,
            dma(n_col - 1, chunks), dma(n_col - 1, chunks),
            dma(n_z - 1, chunks), dma(n_col, chunks), dma(chunks),
            dma(ratio - 1, chunks), dma(ratio - 1, chunks),
            dma(chunks), dma(chunks),
            dma(n_x - 1, chunks), dma(n_x - 1, chunks),
            dma(ratio - 1, chunks), dma(ratio - 1, chunks),
            dma(n_z - 1, chunks), dma(n_z - 1, chunks),
        ],
        compiler_params=pltpu.CompilerParams(collective_id=0, has_side_effects=True),
        name="adjoint",
    )(spectra, window_flags, pair_mask, misfit_weight, observed)
    first, second = pl.pallas_call(
        turn_kernel,
        out_shape=[jax.ShapeDtypeStruct((shard, freqs, width), bf)] * 2,
        in_specs=[pl.BlockSpec(memory_space=pltpu.VMEM)] * 2,
        out_specs=[pl.BlockSpec(memory_space=pltpu.VMEM)] * 2,
        name="turn",
    )(first, second)
    return first, second[None]


def solution(mesh):
    placed = (
        P(("row", "col"), None, None),
        P(("row", "col"), None),
        P("row", "col"),
        P(None, "row", "col"),
        P(None, None, "row", "col"),
    )
    return jax.shard_map(
        functools.partial(per_device, mesh.shape["row"], mesh.shape["col"]),
        mesh=mesh,
        in_specs=placed,
        out_specs=(P(("row", "col"), None, None), P("col", "row", None, None)),
        check_vma=False,
    )
```

```python
import functools

import jax
import jax.numpy as jnp
from jax import lax
from jax.experimental import pallas as pl
from jax.experimental.pallas import tpu as pltpu
from jax.sharding import PartitionSpec as P

MESH = pl.DeviceIdType.MESH
GROUP = 2
LAG_Y, LAG_B, LAG_C = 2, 3, 5


def kernel(
    n_row, n_col, chunks, group,
    raw_hbm, flags_hbm, mask_hbm, w_hbm, obs_hbm, out_first, out_second,
    raw, flags, mask, own,
    v1, v2, w_v, obs_v, gf, gf_sum, rc, rx, sums, halves, last, ry,
    in_sem, own_sem, fs, fr, zs, zr, lz, ys, yr,
    cs, cr, ps, pr, hs, hr, bs, br,
):
    ratio = n_row // n_col
    n_z = n_row // ratio
    n_x = n_col // 2
    bits = n_z.bit_length() - 1
    row, col = lax.axis_index("row"), lax.axis_index("col")
    z, y = row // ratio, row % ratio
    x, core = col // 2, col % 2
    shard = own.shape[1]
    first_rows = n_col * shard
    second_rows = ratio * first_rows
    half = own.shape[2] // 2

    def col_at(step):
        return ((x + step) % n_x) * 2 + core

    partner = x * 2 + (1 - core)

    def row_y(step):
        return z * ratio + (y + step) % ratio

    def row_z(step):
        return ((z + step) % n_z) * ratio + y

    def span(k):
        return pl.ds(k * group, group)

    def remote(src, dst, ssem, rsem, to_row, to_col):
        return pltpu.make_async_remote_copy(
            src_ref=src, dst_ref=dst, send_sem=ssem, recv_sem=rsem,
            device_id=(to_row, to_col), device_id_type=MESH,
        )

    def send_f(k, d):
        return remote(own.at[span(k)], v1.at[span(k), col], fs.at[d - 1], fr.at[k], row, (col + d) % n_col)

    def send_z(k, d):
        return remote(own.at[span(k)], v2.at[span(k), y, col], zs.at[d - 1], zr.at[k], row_z(d), z)

    def send_y(k, d, src):
        return remote(src, v2.at[span(k), y], ys.at[d - 1], yr.at[d - 1, k], row_y(d), col)

    def send_c(k):
        return remote(gf.at[span(k), :, 1 - core], rc.at[span(k)], cs, cr.at[k], row, partner)

    def send_p(k, d):
        return remote(gf_sum.at[span(k), (x + d) % n_x], rx.at[d - 1, span(k)], ps.at[d - 1], pr.at[d - 1, k], row, col_at(d))

    def bit(b):
        return (z // 2**b) % 2

    def row_bit(b):
        return (z + (1 - 2 * bit(b)) * 2**b) * ratio + y

    def send_b(k, b):
        return remote(sums[b].at[span(k), :, 1 - bit(b)], halves[b].at[span(k)], bs.at[b], br.at[b, k], row_bit(b), col)

    def send_h(k, d):
        return remote(last.at[span(k), (y + d) % ratio], ry.at[d - 1, span(k)], hs.at[d - 1], hr.at[d - 1, k], row_y(d), col)

    home = z == col

    load_w = pltpu.make_async_copy(w_hbm, w_v, in_sem.at[0])
    load_obs = pltpu.make_async_copy(obs_hbm, obs_v, in_sem.at[1])
    load_own = pltpu.make_async_copy(own, v1.at[:, col], own_sem)
    load_raw = pltpu.make_async_copy(raw_hbm, raw, in_sem.at[2])
    load_flags = pltpu.make_async_copy(flags_hbm, flags, in_sem.at[3])
    load_mask = pltpu.make_async_copy(mask_hbm, mask, in_sem.at[4])
    load_raw.start()
    load_flags.start()

    barrier = pltpu.get_barrier_semaphore()

    def tell(to_row, to_col):
        pl.semaphore_signal(barrier, inc=1, device_id=(to_row, to_col), device_id_type=MESH)

    @pl.when(jnp.logical_not(home))
    def _():
        for j in range(n_col):
            tell(col * ratio + y, j)

    for b in range(bits):
        tell(row_bit(b), col)
    for d in range(1, ratio):
        tell(row_y(d), col)
    for d in range(1, n_col):
        tell(row, (col + d) % n_col)

    load_raw.wait()
    load_flags.wait()
    load_mask.start()
    load_w.start()
    load_obs.start()
    flag_value = flags[...].astype(jnp.float32)
    flag_both = jnp.concatenate([flag_value, flag_value], axis=1)
    flagged = raw[...].astype(jnp.float32) * flag_both[:, None, :]
    own[...] = jnp.transpose(flagged, (1, 0, 2)).astype(jnp.bfloat16)
    load_own.start()
    pl.semaphore_wait(barrier, n_col - 1 + n_z - 1 + bits + ratio - 1)

    @pl.loop(0, chunks)
    def _(k):
        for d in range(1, n_z):
            send_z(k, d).start()
        for d in range(1, n_col):
            send_f(k, d).start()

    load_own.wait()

    def wait_first(k):
        got = v1.at[span(k), pl.ds(0, n_col - 1)]
        pltpu.make_async_copy(got, got, fr.at[k]).wait()

    def local_copy(k):
        return pltpu.make_async_copy(v1.at[span(k)], v2.at[span(k), y], lz.at[k])

    load_mask.wait()
    load_w.wait()
    load_obs.wait()

    lane = lax.broadcasted_iota(jnp.int32, (1, 2 * half), 1)
    low_plus = jnp.where(lane < half, 1.0, -1.0).astype(jnp.float32)

    def compute(f):
        a = v1[f].astype(jnp.float32).reshape(first_rows, 2 * half)
        b = v2[f].astype(jnp.float32).reshape(second_rows, 2 * half).astype(jnp.bfloat16)
        turned = pltpu.roll(a, half, 1) * low_plus
        w = jnp.concatenate([a, turned], axis=0).astype(jnp.bfloat16)
        cross = lax.dot_general(w, b, (((1,), (1,)), ((), ())), preferred_element_type=jnp.float32)
        scale = mask[...].astype(jnp.float32) * w_v[f].astype(jnp.float32)
        res = jnp.concatenate(
            [
                (scale * (cross[:first_rows] - obs_v[0, f].astype(jnp.float32))).astype(jnp.bfloat16),
                (scale * (cross[first_rows:] - obs_v[1, f].astype(jnp.float32))).astype(jnp.bfloat16),
            ],
            axis=0,
        )
        t = jnp.dot(res, b, preferred_element_type=jnp.float32)
        g1 = t[:first_rows] - pltpu.roll(t[first_rows:], half, 1) * low_plus
        gf[f] = g1.reshape(n_x, 2, shard, 2 * half).astype(jnp.bfloat16)
        g2 = lax.dot_general(res, w, (((0,), (0,)), ((), ())), preferred_element_type=jnp.float32)
        sums[0][f] = g2.reshape(n_z // 2, 2, ratio, shard, 2 * half).astype(jnp.bfloat16)

    lag_y, lag_c = LAG_Y, LAG_C
    lag_b = [lag_y + LAG_B * (b + 1) for b in range(bits)]

    @pl.loop(0, chunks + max(lag_b[-1], lag_c))
    def _(it):
        @pl.when(it < chunks)
        def _():
            @pl.when(home)
            def _():
                wait_first(it)
                for d in range(1, ratio):
                    send_y(it, d, v1.at[span(it)]).start()
                local_copy(it).start()

            @pl.when(jnp.logical_not(home))
            def _():
                got = v2.at[span(it), y]
                pltpu.make_async_copy(got, got, zr.at[it]).wait()
                for d in range(1, ratio):
                    send_y(it, d, v2.at[span(it), y]).start()

        @pl.when(jnp.logical_and(it >= lag_y, it < chunks + lag_y))
        def _():
            k = it - lag_y
            for d in range(1, ratio):
                send_y(k, d, v2.at[span(k), y]).wait_recv()

            @pl.when(home)
            def _():
                local_copy(k).wait()

            @pl.when(jnp.logical_not(home))
            def _():
                wait_first(k)

            for i in range(group):
                compute(k * group + i)
            send_c(k).start()
            send_b(k, 0).start()

        for b in range(bits):
            @pl.when(jnp.logical_and(it >= lag_b[b], it < chunks + lag_b[b]))
            def _():
                k = it - lag_b[b]
                send_b(k, b).wait_recv()
                total = sums[b][span(k), :, bit(b)].astype(jnp.float32) + halves[b][span(k)].astype(jnp.float32)
                if b + 1 < bits:
                    sums[b + 1][span(k)] = total.reshape(
                        group, n_z // 2 ** (b + 2), 2, ratio, shard, 2 * half
                    ).astype(jnp.bfloat16)
                    send_b(k, b + 1).start()
                else:
                    last[span(k)] = total[:, 0].astype(jnp.bfloat16)
                    for d in range(1, ratio):
                        send_h(k, d).start()

        @pl.when(jnp.logical_and(it >= lag_c, it < chunks + lag_c))
        def _():
            k = it - lag_c
            send_c(k).wait_recv()
            total = gf[span(k), :, core].astype(jnp.float32) + rc[span(k)].astype(jnp.float32)
            gf_sum[span(k)] = total.astype(jnp.bfloat16)
            for d in range(1, n_x):
                send_p(k, d).start()

    @pl.loop(0, chunks)
    def _(k):
        for d in range(1, n_x):
            send_p(k, d).wait_recv()
        total = gf_sum[span(k), x].astype(jnp.float32)
        for d in range(1, n_x):
            total = total + rx[d - 1, span(k)].astype(jnp.float32)
        out_first[span(k)] = total.astype(jnp.bfloat16)
        total = last[span(k), y].astype(jnp.float32)
        for d in range(1, ratio):
            send_h(k, d).wait_recv()
            total = total + ry[d - 1, span(k)].astype(jnp.float32)
        out_second[span(k)] = total.astype(jnp.bfloat16)

    def sent(ref, sem):
        pltpu.make_async_copy(ref, ref, sem).wait()

    for d in range(1, n_col):
        sent(own, fs.at[d - 1])
    for d in range(1, n_z):
        sent(own, zs.at[d - 1])
    for d in range(1, ratio):
        sent(v1, ys.at[d - 1])
        sent(own, hs.at[d - 1])
    for d in range(1, n_x):
        sent(own, ps.at[d - 1])
    sent(rc, cs)
    for b in range(bits):
        sent(halves[b], bs.at[b])


def turn_kernel(first, second, out_first, out_second):
    for src, dst in ((first, out_first), (second, out_second)):
        dst[...] = jnp.transpose(src[...].astype(jnp.float32), (1, 0, 2)).astype(jnp.bfloat16)


def per_device(n_row, n_col, spectra, window_flags, pair_mask, misfit_weight, observed):
    shard, freqs, width = spectra.shape
    ratio = n_row // n_col
    n_z, n_x = n_row // ratio, n_col // 2
    bits = n_z.bit_length() - 1
    group = GROUP if freqs % GROUP == 0 else 1
    chunks = freqs // group
    bf = jnp.bfloat16
    vm = lambda *shape: pltpu.VMEM(shape, bf)
    dma = lambda *shape: pltpu.SemaphoreType.DMA(shape)
    first, second = pl.pallas_call(
        functools.partial(kernel, n_row, n_col, chunks, group),
        out_shape=[jax.ShapeDtypeStruct((freqs, shard, width), bf)] * 2,
        in_specs=[
            pl.BlockSpec(memory_space=pl.ANY),
        ] * 5,
        out_specs=[pl.BlockSpec(memory_space=pltpu.VMEM)] * 2,
        scratch_shapes=[
            pltpu.VMEM(spectra.shape, bf),
            pltpu.VMEM(window_flags.shape, window_flags.dtype),
            pltpu.VMEM(pair_mask.shape, pair_mask.dtype),
            vm(freqs, shard, width),
            vm(freqs, n_col, shard, width),
            vm(freqs, ratio, n_col, shard, width),
            pltpu.VMEM(misfit_weight.shape, bf),
            pltpu.VMEM(observed.shape, bf),
            vm(freqs, n_x, 2, shard, width),
            vm(freqs, n_x, shard, width),
            vm(freqs, n_x, shard, width),
            vm(n_x - 1, freqs, shard, width),
            [vm(freqs, n_z // 2 ** (b + 1), 2, ratio, shard, width) for b in range(bits)],
            [vm(freqs, n_z // 2 ** (b + 1), ratio, shard, width) for b in range(bits)],
            vm(freqs, ratio, shard, width),
            vm(ratio - 1, freqs, shard, width),
            dma(5), pltpu.SemaphoreType.DMA,
            dma(n_col - 1), dma(chunks),
            dma(n_z - 1), dma(chunks), dma(chunks),
            dma(ratio - 1), dma(ratio - 1, chunks),
            pltpu.SemaphoreType.DMA, dma(chunks),
            dma(n_x - 1), dma(n_x - 1, chunks),
            dma(ratio - 1), dma(ratio - 1, chunks),
            dma(bits), dma(bits, chunks),
        ],
        compiler_params=pltpu.CompilerParams(collective_id=0, has_side_effects=True),
        name="adjoint",
    )(spectra, window_flags, pair_mask, misfit_weight, observed)
    first, second = pl.pallas_call(
        turn_kernel,
        out_shape=[jax.ShapeDtypeStruct((shard, freqs, width), bf)] * 2,
        in_specs=[pl.BlockSpec(memory_space=pltpu.VMEM)] * 2,
        out_specs=[pl.BlockSpec(memory_space=pltpu.VMEM)] * 2,
        name="turn",
    )(first, second)
    return first, second[None]


def solution(mesh):
    placed = (
        P(("row", "col"), None, None),
        P(("row", "col"), None),
        P("row", "col"),
        P(None, "row", "col"),
        P(None, None, "row", "col"),
    )
    return jax.shard_map(
        functools.partial(per_device, mesh.shape["row"], mesh.shape["col"]),
        mesh=mesh,
        in_specs=placed,
        out_specs=(P(("row", "col"), None, None), P("col", "row", None, None)),
        check_vma=False,
    )
```

```python
import functools

import jax
import jax.numpy as jnp
from jax import lax
from jax.experimental import pallas as pl
from jax.experimental.pallas import tpu as pltpu
from jax.sharding import PartitionSpec as P

MESH = pl.DeviceIdType.MESH
GROUP = 2
LAG_Y, LAG_B, LAG_C = 3, 3, 7


def kernel(
    n_row, n_col, chunks, group,
    raw_hbm, flags_hbm, mask_hbm, w_hbm, obs_hbm, out_first, out_second,
    raw, flags, mask, own,
    v1, v2, w_v, obs_v, gf, gf_sum, rc, rx, sums, halves, last, ry,
    in_sem, own_sem, fs, fr, zs, zr, lz, ys, yr,
    cs, cr, ps, pr, hs, hr, bs, br,
):
    ratio = n_row // n_col
    n_z = n_row // ratio
    n_x = n_col // 2
    bits = n_z.bit_length() - 1
    row, col = lax.axis_index("row"), lax.axis_index("col")
    z, y = row // ratio, row % ratio
    x, core = col // 2, col % 2
    shard = own.shape[1]
    first_rows = n_col * shard
    second_rows = ratio * first_rows
    half = own.shape[2] // 2

    def col_at(step):
        return ((x + step) % n_x) * 2 + core

    partner = x * 2 + (1 - core)

    def row_y(step):
        return z * ratio + (y + step) % ratio

    def row_z(step):
        return ((z + step) % n_z) * ratio + y

    def span(k):
        return pl.ds(k * group, group)

    def remote(src, dst, ssem, rsem, to_row, to_col):
        return pltpu.make_async_remote_copy(
            src_ref=src, dst_ref=dst, send_sem=ssem, recv_sem=rsem,
            device_id=(to_row, to_col), device_id_type=MESH,
        )

    def send_f(k, d):
        return remote(own.at[span(k)], v1.at[span(k), col], fs.at[d - 1], fr.at[k], row, (col + d) % n_col)

    def send_z(k, d):
        return remote(own.at[span(k)], v2.at[span(k), y, col], zs.at[d - 1], zr.at[k], row_z(d), z)

    def send_y(k, d, src):
        return remote(src, v2.at[span(k), y], ys.at[d - 1], yr.at[d - 1, k], row_y(d), col)

    def send_c(k):
        return remote(gf.at[span(k), :, 1 - core], rc.at[span(k)], cs, cr.at[k], row, partner)

    def send_p(k, d):
        return remote(gf_sum.at[span(k), (x + d) % n_x], rx.at[d - 1, span(k)], ps.at[d - 1], pr.at[d - 1, k], row, col_at(d))

    def bit(b):
        return (z // 2**b) % 2

    def row_bit(b):
        return (z + (1 - 2 * bit(b)) * 2**b) * ratio + y

    def send_b(k, b):
        return remote(sums[b].at[span(k), :, 1 - bit(b)], halves[b].at[span(k)], bs.at[b], br.at[b, k], row_bit(b), col)

    def send_h(k, d):
        return remote(last.at[span(k), (y + d) % ratio], ry.at[d - 1, span(k)], hs.at[d - 1], hr.at[d - 1, k], row_y(d), col)

    home = z == col

    load_w = pltpu.make_async_copy(w_hbm, w_v, in_sem.at[0])
    load_obs = pltpu.make_async_copy(obs_hbm, obs_v, in_sem.at[1])
    load_own = pltpu.make_async_copy(own, v1.at[:, col], own_sem)
    load_raw = pltpu.make_async_copy(raw_hbm, raw, in_sem.at[2])
    load_flags = pltpu.make_async_copy(flags_hbm, flags, in_sem.at[3])
    load_mask = pltpu.make_async_copy(mask_hbm, mask, in_sem.at[4])
    load_raw.start()
    load_flags.start()

    barrier = pltpu.get_barrier_semaphore()

    def tell(to_row, to_col):
        pl.semaphore_signal(barrier, inc=1, device_id=(to_row, to_col), device_id_type=MESH)

    @pl.when(jnp.logical_not(home))
    def _():
        for j in range(n_col):
            tell(col * ratio + y, j)

    for b in range(bits):
        tell(row_bit(b), col)
    for d in range(1, ratio):
        tell(row_y(d), col)
    for d in range(1, n_col):
        tell(row, (col + d) % n_col)

    load_raw.wait()
    load_flags.wait()
    load_mask.start()
    load_w.start()
    load_obs.start()
    flag_value = flags[...].astype(jnp.float32)
    flag_both = jnp.concatenate([flag_value, flag_value], axis=1)
    flagged = raw[...].astype(jnp.float32) * flag_both[:, None, :]
    own[...] = jnp.transpose(flagged, (1, 0, 2)).astype(jnp.bfloat16)
    load_own.start()
    pl.semaphore_wait(barrier, n_col - 1 + n_z - 1 + bits + ratio - 1)

    @pl.loop(0, chunks)
    def _(k):
        for d in range(n_z - 1, 0, -1):
            send_z(k, d).start()
        for d in range(1, n_col):
            send_f(k, d).start()

    load_own.wait()

    def wait_first(k):
        got = v1.at[span(k), pl.ds(0, n_col - 1)]
        pltpu.make_async_copy(got, got, fr.at[k]).wait()

    def local_copy(k):
        return pltpu.make_async_copy(v1.at[span(k)], v2.at[span(k), y], lz.at[k])

    lane = lax.broadcasted_iota(jnp.int32, (1, 2 * half), 1)
    low_plus = jnp.where(lane < half, 1.0, -1.0).astype(jnp.float32)

    def compute(f):
        a = v1[f].astype(jnp.float32).reshape(first_rows, 2 * half)
        b = v2[f].astype(jnp.float32).reshape(second_rows, 2 * half).astype(jnp.bfloat16)
        turned = pltpu.roll(a, half, 1) * low_plus
        w = jnp.concatenate([a, turned], axis=0).astype(jnp.bfloat16)
        cross = lax.dot_general(w, b, (((1,), (1,)), ((), ())), preferred_element_type=jnp.float32)
        scale = mask[...].astype(jnp.float32) * w_v[f].astype(jnp.float32)
        res = jnp.concatenate(
            [
                (scale * (cross[:first_rows] - obs_v[0, f].astype(jnp.float32))).astype(jnp.bfloat16),
                (scale * (cross[first_rows:] - obs_v[1, f].astype(jnp.float32))).astype(jnp.bfloat16),
            ],
            axis=0,
        )
        t = jnp.dot(res, b, preferred_element_type=jnp.float32)
        g1 = t[:first_rows] - pltpu.roll(t[first_rows:], half, 1) * low_plus
        gf[f] = g1.reshape(n_x, 2, shard, 2 * half).astype(jnp.bfloat16)
        g2 = lax.dot_general(res, w, (((0,), (0,)), ((), ())), preferred_element_type=jnp.float32)
        sums[0][f] = g2.reshape(n_z // 2, 2, ratio, shard, 2 * half).astype(jnp.bfloat16)

    lag_y, lag_c = LAG_Y, LAG_C
    lag_b = [lag_y + LAG_B * (b + 1) for b in range(bits)]

    @pl.loop(0, chunks + max(lag_b[-1], lag_c))
    def _(it):
        @pl.when(it < chunks)
        def _():
            @pl.when(home)
            def _():
                wait_first(it)
                for d in range(1, ratio):
                    send_y(it, d, v1.at[span(it)]).start()
                local_copy(it).start()

            @pl.when(jnp.logical_not(home))
            def _():
                got = v2.at[span(it), y]
                pltpu.make_async_copy(got, got, zr.at[it]).wait()
                for d in range(1, ratio):
                    send_y(it, d, v2.at[span(it), y]).start()

        @pl.when(jnp.logical_and(it >= lag_y, it < chunks + lag_y))
        def _():
            k = it - lag_y

            @pl.when(k == 0)
            def _():
                load_mask.wait()
                load_w.wait()
                load_obs.wait()

            for d in range(1, ratio):
                send_y(k, d, v2.at[span(k), y]).wait_recv()

            @pl.when(home)
            def _():
                local_copy(k).wait()

            @pl.when(jnp.logical_not(home))
            def _():
                wait_first(k)

            for i in range(group):
                compute(k * group + i)
            send_c(k).start()
            send_b(k, 0).start()

        for b in range(bits):
            @pl.when(jnp.logical_and(it >= lag_b[b], it < chunks + lag_b[b]))
            def _():
                k = it - lag_b[b]
                send_b(k, b).wait_recv()
                total = sums[b][span(k), :, bit(b)].astype(jnp.float32) + halves[b][span(k)].astype(jnp.float32)
                if b + 1 < bits:
                    sums[b + 1][span(k)] = total.reshape(
                        group, n_z // 2 ** (b + 2), 2, ratio, shard, 2 * half
                    ).astype(jnp.bfloat16)
                    send_b(k, b + 1).start()
                else:
                    last[span(k)] = total[:, 0].astype(jnp.bfloat16)
                    for d in range(1, ratio):
                        send_h(k, d).start()

        @pl.when(jnp.logical_and(it >= lag_c, it < chunks + lag_c))
        def _():
            k = it - lag_c
            send_c(k).wait_recv()
            total = gf[span(k), :, core].astype(jnp.float32) + rc[span(k)].astype(jnp.float32)
            gf_sum[span(k)] = total.astype(jnp.bfloat16)
            for d in range(1, n_x):
                send_p(k, d).start()

    @pl.loop(0, chunks)
    def _(k):
        for d in range(1, n_x):
            send_p(k, d).wait_recv()
        total = gf_sum[span(k), x].astype(jnp.float32)
        for d in range(1, n_x):
            total = total + rx[d - 1, span(k)].astype(jnp.float32)
        out_first[span(k)] = total.astype(jnp.bfloat16)
        total = last[span(k), y].astype(jnp.float32)
        for d in range(1, ratio):
            send_h(k, d).wait_recv()
            total = total + ry[d - 1, span(k)].astype(jnp.float32)
        out_second[span(k)] = total.astype(jnp.bfloat16)

    def sent(ref, sem):
        pltpu.make_async_copy(ref, ref, sem).wait()

    for d in range(1, n_col):
        sent(own, fs.at[d - 1])
    for d in range(1, n_z):
        sent(own, zs.at[d - 1])
    for d in range(1, ratio):
        sent(v1, ys.at[d - 1])
        sent(own, hs.at[d - 1])
    for d in range(1, n_x):
        sent(own, ps.at[d - 1])
    sent(rc, cs)
    for b in range(bits):
        sent(halves[b], bs.at[b])


def turn_kernel(first, second, out_first, out_second):
    for src, dst in ((first, out_first), (second, out_second)):
        dst[...] = jnp.transpose(src[...].astype(jnp.float32), (1, 0, 2)).astype(jnp.bfloat16)


def per_device(n_row, n_col, spectra, window_flags, pair_mask, misfit_weight, observed):
    shard, freqs, width = spectra.shape
    ratio = n_row // n_col
    n_z, n_x = n_row // ratio, n_col // 2
    bits = n_z.bit_length() - 1
    group = GROUP if freqs % GROUP == 0 else 1
    chunks = freqs // group
    bf = jnp.bfloat16
    vm = lambda *shape: pltpu.VMEM(shape, bf)
    dma = lambda *shape: pltpu.SemaphoreType.DMA(shape)
    first, second = pl.pallas_call(
        functools.partial(kernel, n_row, n_col, chunks, group),
        out_shape=[jax.ShapeDtypeStruct((freqs, shard, width), bf)] * 2,
        in_specs=[
            pl.BlockSpec(memory_space=pl.ANY),
        ] * 5,
        out_specs=[pl.BlockSpec(memory_space=pltpu.VMEM)] * 2,
        scratch_shapes=[
            pltpu.VMEM(spectra.shape, bf),
            pltpu.VMEM(window_flags.shape, window_flags.dtype),
            pltpu.VMEM(pair_mask.shape, pair_mask.dtype),
            vm(freqs, shard, width),
            vm(freqs, n_col, shard, width),
            vm(freqs, ratio, n_col, shard, width),
            pltpu.VMEM(misfit_weight.shape, bf),
            pltpu.VMEM(observed.shape, bf),
            vm(freqs, n_x, 2, shard, width),
            vm(freqs, n_x, shard, width),
            vm(freqs, n_x, shard, width),
            vm(n_x - 1, freqs, shard, width),
            [vm(freqs, n_z // 2 ** (b + 1), 2, ratio, shard, width) for b in range(bits)],
            [vm(freqs, n_z // 2 ** (b + 1), ratio, shard, width) for b in range(bits)],
            vm(freqs, ratio, shard, width),
            vm(ratio - 1, freqs, shard, width),
            dma(5), pltpu.SemaphoreType.DMA,
            dma(n_col - 1), dma(chunks),
            dma(n_z - 1), dma(chunks), dma(chunks),
            dma(ratio - 1), dma(ratio - 1, chunks),
            pltpu.SemaphoreType.DMA, dma(chunks),
            dma(n_x - 1), dma(n_x - 1, chunks),
            dma(ratio - 1), dma(ratio - 1, chunks),
            dma(bits), dma(bits, chunks),
        ],
        compiler_params=pltpu.CompilerParams(collective_id=0, has_side_effects=True),
        name="adjoint",
    )(spectra, window_flags, pair_mask, misfit_weight, observed)
    parts = 2 if shard % 32 == 0 else 1
    first, second = pl.pallas_call(
        turn_kernel,
        out_shape=[jax.ShapeDtypeStruct((shard, freqs, width), bf)] * 2,
        grid=(parts,),
        in_specs=[pl.BlockSpec((freqs, shard // parts, width), lambda i: (0, i, 0))] * 2,
        out_specs=[pl.BlockSpec((shard // parts, freqs, width), lambda i: (i, 0, 0))] * 2,
        name="turn",
    )(first, second)
    return first, second[None]


def solution(mesh):
    placed = (
        P(("row", "col"), None, None),
        P(("row", "col"), None),
        P("row", "col"),
        P(None, "row", "col"),
        P(None, None, "row", "col"),
    )
    return jax.shard_map(
        functools.partial(per_device, mesh.shape["row"], mesh.shape["col"]),
        mesh=mesh,
        in_specs=placed,
        out_specs=(P(("row", "col"), None, None), P("col", "row", None, None)),
        check_vma=False,
    )
```

```python
import functools

import jax
import jax.numpy as jnp
from jax import lax
from jax.experimental import pallas as pl
from jax.experimental.pallas import tpu as pltpu
from jax.sharding import PartitionSpec as P

MESH = pl.DeviceIdType.MESH
GROUP = 2
LAG_Y, LAG_B, LAG_C = 3, 3, 7


def kernel(
    n_row, n_col, chunks, group,
    raw_hbm, flags_hbm, mask_hbm, w_hbm, obs_hbm, out_first, out_second,
    raw, flags, mask, own,
    v1, v2, w_v, obs_v, gf, gf_sum, rc, rx, sums, halves, last, ry,
    in_sem, own_sem, fs, fr, zs, zr, lz, ys, yr,
    cs, cr, ps, pr, hs, hr, bs, br,
):
    ratio = n_row // n_col
    n_z = n_row // ratio
    n_x = n_col // 2
    bits = n_z.bit_length() - 1
    row, col = lax.axis_index("row"), lax.axis_index("col")
    z, y = row // ratio, row % ratio
    x, core = col // 2, col % 2
    shard = own.shape[1]
    first_rows = n_col * shard
    second_rows = ratio * first_rows
    half = own.shape[2] // 2

    def col_at(step):
        return ((x + step) % n_x) * 2 + core

    partner = x * 2 + (1 - core)

    def row_y(step):
        return z * ratio + (y + step) % ratio

    def row_z(step):
        return ((z + step) % n_z) * ratio + y

    def span(k):
        return pl.ds(k * group, group)

    def remote(src, dst, ssem, rsem, to_row, to_col):
        return pltpu.make_async_remote_copy(
            src_ref=src, dst_ref=dst, send_sem=ssem, recv_sem=rsem,
            device_id=(to_row, to_col), device_id_type=MESH,
        )

    def send_f(k, d):
        return remote(own.at[span(k)], v1.at[span(k), col], fs.at[d - 1], fr.at[k], row, (col + d) % n_col)

    def send_z(k, d):
        return remote(own.at[span(k)], v2.at[span(k), y, col], zs.at[d - 1], zr.at[k], row_z(d), z)

    def send_y(k, d, src):
        return remote(src, v2.at[span(k), y], ys.at[d - 1], yr.at[d - 1, k], row_y(d), col)

    def send_c(k):
        return remote(gf.at[span(k), :, 1 - core], rc.at[span(k)], cs, cr.at[k], row, partner)

    def send_p(k, d):
        return remote(gf_sum.at[span(k), (x + d) % n_x], rx.at[d - 1, span(k)], ps.at[d - 1], pr.at[d - 1, k], row, col_at(d))

    def bit(b):
        return (z // 2**b) % 2

    def row_bit(b):
        return (z + (1 - 2 * bit(b)) * 2**b) * ratio + y

    def send_b(k, b):
        return remote(sums[b].at[span(k), :, 1 - bit(b)], halves[b].at[span(k)], bs.at[b], br.at[b, k], row_bit(b), col)

    def send_h(k, d):
        return remote(last.at[span(k), (y + d) % ratio], ry.at[d - 1, span(k)], hs.at[d - 1], hr.at[d - 1, k], row_y(d), col)

    home = z == col

    load_w = pltpu.make_async_copy(w_hbm, w_v, in_sem.at[0])
    load_obs = pltpu.make_async_copy(obs_hbm, obs_v, in_sem.at[1])
    load_own = pltpu.make_async_copy(own, v1.at[:, col], own_sem)
    load_raw = pltpu.make_async_copy(raw_hbm, raw, in_sem.at[2])
    load_flags = pltpu.make_async_copy(flags_hbm, flags, in_sem.at[3])
    load_mask = pltpu.make_async_copy(mask_hbm, mask, in_sem.at[4])
    load_raw.start()
    load_flags.start()

    barrier = pltpu.get_barrier_semaphore()

    def tell(to_row, to_col):
        pl.semaphore_signal(barrier, inc=1, device_id=(to_row, to_col), device_id_type=MESH)

    @pl.when(jnp.logical_not(home))
    def _():
        for j in range(n_col):
            tell(col * ratio + y, j)

    for b in range(bits):
        tell(row_bit(b), col)
    for d in range(1, ratio):
        tell(row_y(d), col)
    for d in range(1, n_col):
        tell(row, (col + d) % n_col)

    load_raw.wait()
    load_flags.wait()
    load_mask.start()
    load_w.start()
    load_obs.start()
    flag_value = flags[...].astype(jnp.float32)
    flag_both = jnp.concatenate([flag_value, flag_value], axis=1)
    flagged = raw[...].astype(jnp.float32) * flag_both[:, None, :]
    own[...] = jnp.transpose(flagged, (1, 0, 2)).astype(jnp.bfloat16)
    load_own.start()
    pl.semaphore_wait(barrier, n_col - 1 + n_z - 1 + bits + ratio - 1)

    @pl.loop(0, chunks)
    def _(k):
        for d in range(n_z - 1, 0, -1):
            send_z(k, d).start()
        for d in range(1, n_col):
            send_f(k, d).start()

    load_own.wait()

    def wait_first(k):
        got = v1.at[span(k), pl.ds(0, n_col - 1)]
        pltpu.make_async_copy(got, got, fr.at[k]).wait()

    def local_copy(k):
        return pltpu.make_async_copy(v1.at[span(k)], v2.at[span(k), y], lz.at[k])

    lane = lax.broadcasted_iota(jnp.int32, (1, 2 * half), 1)
    low_plus = jnp.where(lane < half, 1.0, -1.0).astype(jnp.float32)

    def compute(f):
        a = v1[f].astype(jnp.float32).reshape(first_rows, 2 * half)
        b = v2[f].astype(jnp.float32).reshape(second_rows, 2 * half).astype(jnp.bfloat16)
        turned = pltpu.roll(a, half, 1) * low_plus
        w = jnp.concatenate([a, turned], axis=0).astype(jnp.bfloat16)
        cross = lax.dot_general(w, b, (((1,), (1,)), ((), ())), preferred_element_type=jnp.float32)
        scale = mask[...].astype(jnp.float32) * w_v[f].astype(jnp.float32)
        res = jnp.concatenate(
            [
                (scale * (cross[:first_rows] - obs_v[0, f].astype(jnp.float32))).astype(jnp.bfloat16),
                (scale * (cross[first_rows:] - obs_v[1, f].astype(jnp.float32))).astype(jnp.bfloat16),
            ],
            axis=0,
        )
        t = jnp.dot(res, b, preferred_element_type=jnp.float32)
        g1 = t[:first_rows] - pltpu.roll(t[first_rows:], half, 1) * low_plus
        gf[f] = g1.reshape(n_x, 2, shard, 2 * half).astype(jnp.bfloat16)
        g2 = lax.dot_general(res, w, (((0,), (0,)), ((), ())), preferred_element_type=jnp.float32)
        sums[0][f] = g2.reshape(n_z // 2, 2, ratio, shard, 2 * half).astype(jnp.bfloat16)

    lag_y, lag_c = LAG_Y, LAG_C
    lag_b = [lag_y + LAG_B * (b + 1) for b in range(bits)]

    @pl.loop(0, chunks + max(lag_b[-1], lag_c))
    def _(it):
        @pl.when(it < chunks)
        def _():
            @pl.when(home)
            def _():
                wait_first(it)
                for d in range(1, ratio):
                    send_y(it, d, v1.at[span(it)]).start()
                local_copy(it).start()

            @pl.when(jnp.logical_not(home))
            def _():
                got = v2.at[span(it), y]
                pltpu.make_async_copy(got, got, zr.at[it]).wait()
                for d in range(1, ratio):
                    send_y(it, d, v2.at[span(it), y]).start()

        @pl.when(jnp.logical_and(it >= lag_y, it < chunks + lag_y))
        def _():
            k = it - lag_y

            @pl.when(k == 0)
            def _():
                load_mask.wait()
                load_w.wait()
                load_obs.wait()

            for d in range(1, ratio):
                send_y(k, d, v2.at[span(k), y]).wait_recv()

            @pl.when(home)
            def _():
                local_copy(k).wait()

            @pl.when(jnp.logical_not(home))
            def _():
                wait_first(k)

            for i in range(group):
                compute(k * group + i)
            send_b(k, 0).start()
            send_c(k).start()

        for b in range(bits):
            @pl.when(jnp.logical_and(it >= lag_b[b], it < chunks + lag_b[b]))
            def _():
                k = it - lag_b[b]
                send_b(k, b).wait_recv()
                total = sums[b][span(k), :, bit(b)].astype(jnp.float32) + halves[b][span(k)].astype(jnp.float32)
                if b + 1 < bits:
                    sums[b + 1][span(k)] = total.reshape(
                        group, n_z // 2 ** (b + 2), 2, ratio, shard, 2 * half
                    ).astype(jnp.bfloat16)
                    send_b(k, b + 1).start()
                else:
                    last[span(k)] = total[:, 0].astype(jnp.bfloat16)
                    for d in range(1, ratio):
                        send_h(k, d).start()

        @pl.when(jnp.logical_and(it >= lag_c, it < chunks + lag_c))
        def _():
            k = it - lag_c
            send_c(k).wait_recv()
            total = gf[span(k), :, core].astype(jnp.float32) + rc[span(k)].astype(jnp.float32)
            gf_sum[span(k)] = total.astype(jnp.bfloat16)
            for d in range(1, n_x):
                send_p(k, d).start()

    @pl.loop(0, chunks)
    def _(k):
        for d in range(1, n_x):
            send_p(k, d).wait_recv()
        total = gf_sum[span(k), x].astype(jnp.float32)
        for d in range(1, n_x):
            total = total + rx[d - 1, span(k)].astype(jnp.float32)
        out_first[span(k)] = total.astype(jnp.bfloat16)
        total = last[span(k), y].astype(jnp.float32)
        for d in range(1, ratio):
            send_h(k, d).wait_recv()
            total = total + ry[d - 1, span(k)].astype(jnp.float32)
        out_second[span(k)] = total.astype(jnp.bfloat16)

    def sent(ref, sem):
        pltpu.make_async_copy(ref, ref, sem).wait()

    for d in range(1, n_col):
        sent(own, fs.at[d - 1])
    for d in range(1, n_z):
        sent(own, zs.at[d - 1])
    for d in range(1, ratio):
        sent(v1, ys.at[d - 1])
        sent(own, hs.at[d - 1])
    for d in range(1, n_x):
        sent(own, ps.at[d - 1])
    sent(rc, cs)
    for b in range(bits):
        sent(halves[b], bs.at[b])


def turn_kernel(first, second, out_first, out_second):
    for src, dst in ((first, out_first), (second, out_second)):
        dst[...] = jnp.transpose(src[...].astype(jnp.float32), (1, 0, 2)).astype(jnp.bfloat16)


def per_device(n_row, n_col, spectra, window_flags, pair_mask, misfit_weight, observed):
    shard, freqs, width = spectra.shape
    ratio = n_row // n_col
    n_z, n_x = n_row // ratio, n_col // 2
    bits = n_z.bit_length() - 1
    group = GROUP if freqs % GROUP == 0 else 1
    chunks = freqs // group
    bf = jnp.bfloat16
    vm = lambda *shape: pltpu.VMEM(shape, bf)
    dma = lambda *shape: pltpu.SemaphoreType.DMA(shape)
    first, second = pl.pallas_call(
        functools.partial(kernel, n_row, n_col, chunks, group),
        out_shape=[jax.ShapeDtypeStruct((freqs, shard, width), bf)] * 2,
        in_specs=[
            pl.BlockSpec(memory_space=pl.ANY),
        ] * 5,
        out_specs=[pl.BlockSpec(memory_space=pltpu.VMEM)] * 2,
        scratch_shapes=[
            pltpu.VMEM(spectra.shape, bf),
            pltpu.VMEM(window_flags.shape, window_flags.dtype),
            pltpu.VMEM(pair_mask.shape, pair_mask.dtype),
            vm(freqs, shard, width),
            vm(freqs, n_col, shard, width),
            vm(freqs, ratio, n_col, shard, width),
            pltpu.VMEM(misfit_weight.shape, bf),
            pltpu.VMEM(observed.shape, bf),
            vm(freqs, n_x, 2, shard, width),
            vm(freqs, n_x, shard, width),
            vm(freqs, n_x, shard, width),
            vm(n_x - 1, freqs, shard, width),
            [vm(freqs, n_z // 2 ** (b + 1), 2, ratio, shard, width) for b in range(bits)],
            [vm(freqs, n_z // 2 ** (b + 1), ratio, shard, width) for b in range(bits)],
            vm(freqs, ratio, shard, width),
            vm(ratio - 1, freqs, shard, width),
            dma(5), pltpu.SemaphoreType.DMA,
            dma(n_col - 1), dma(chunks),
            dma(n_z - 1), dma(chunks), dma(chunks),
            dma(ratio - 1), dma(ratio - 1, chunks),
            pltpu.SemaphoreType.DMA, dma(chunks),
            dma(n_x - 1), dma(n_x - 1, chunks),
            dma(ratio - 1), dma(ratio - 1, chunks),
            dma(bits), dma(bits, chunks),
        ],
        compiler_params=pltpu.CompilerParams(collective_id=0, has_side_effects=True),
        name="adjoint",
    )(spectra, window_flags, pair_mask, misfit_weight, observed)
    parts = 2 if shard % 32 == 0 else 1
    first, second = pl.pallas_call(
        turn_kernel,
        out_shape=[jax.ShapeDtypeStruct((shard, freqs, width), bf)] * 2,
        grid=(parts,),
        in_specs=[pl.BlockSpec((freqs, shard // parts, width), lambda i: (0, i, 0))] * 2,
        out_specs=[pl.BlockSpec((shard // parts, freqs, width), lambda i: (i, 0, 0))] * 2,
        name="turn",
    )(first, second)
    return first, second[None]


def solution(mesh):
    placed = (
        P(("row", "col"), None, None),
        P(("row", "col"), None),
        P("row", "col"),
        P(None, "row", "col"),
        P(None, None, "row", "col"),
    )
    return jax.shard_map(
        functools.partial(per_device, mesh.shape["row"], mesh.shape["col"]),
        mesh=mesh,
        in_specs=placed,
        out_specs=(P(("row", "col"), None, None), P("col", "row", None, None)),
        check_vma=False,
    )
```
